128 devices in a mesh: grp: 16 (over x_lo, z, core), rep: 8 (over y, x_hi).
Axes of the slice: x: 4 (x_hi: 2, x_lo: 2; x = x_hi * 2 + x_lo), y: 4, z: 4, core: 2. Of those that a mesh axis runs over, the one named last changes fastest.
Arguments:
- queries: bfloat16 [49152, 2560], P(('grp', 'rep')), may hold values from -60 to 60
- passages: bfloat16 [262144, 2560], P(('grp', 'rep')), may hold values from -60 to 60
- block_valid_counts: int32 [2048], P(('grp', 'rep')), may hold values from 16 to 128
- positive_index: int32 [49152], P(('grp', 'rep')), may hold values from 0 to 2047, as said below
- neg_blocks: int32 [128, 28], P(('grp', 'rep')), may hold values from 0 to 2047, as said below
- query_weights: float32 [49152], P(('grp', 'rep')), may hold values from 0.3 to 10
Outputs:
- query_loss: float32 [49152], P(('grp', 'rep'))
- mean_loss: float32 [], replicated
The draws below stay inside these ranges and needn't reach their ends.
Inputs may be any that keep to these rules, and one draw needn't show every extreme that they name: `neg_blocks`: row g lists 28 distinct blocks, all owned by query groups with the same rep index as group g and another grp index; at most 2 of them belong to one group, and some group gives exactly 2 in every row. `positive_index`: always a valid row of one of the query's own group's blocks.
All inputs are finite; a program needn't handle non-finite values.
Results may differ from the reference program's by a relative error of at most 0.0003.
Values may be sent and summed in bfloat16 or wider, within the bound.
No kernel may reach another device: no remote copies, remote signals or barrier semaphores. Data moves between devices by JAX's collectives and lax.ppermute only.
A program may use at most 256 MiB of HBM per device.

```python
import jax
import jax.numpy as jnp
from jax import lax

D = 2560
QG = 384
BPD = 16
BR = 128
CAP = 2
NEG = 28
QUERIES = 49152
NBLOCKS = 2048
PASSAGES = 262144
N_GRP = 16
N_REP = 8


cluster_count = 32


def cluster_rows(key, rows, salt):
    centers = jax.random.normal(jax.random.fold_in(key, 101), (cluster_count, D), jnp.float32)
    column_scale = jnp.exp(jax.random.uniform(jax.random.fold_in(key, 102), (D,), jnp.float32, -1.15, 1.15))
    own_key = jax.random.fold_in(key, salt)
    key_labels, target_length_factor, key_noise = jax.random.split(own_key, 3)
    labels = jax.random.randint(key_labels, (rows,), 0, cluster_count)
    row_scale = jnp.exp(jax.random.uniform(target_length_factor, (rows, 1), jnp.float32, -1.15, 1.15))
    noise = jax.random.normal(key_noise, (rows, D), jnp.float32)
    member = jnp.take(centers, labels, axis=0)
    return jnp.clip(row_scale * (member + noise * column_scale), -60.0, 60.0)


def draw_queries(key, part):
    return cluster_rows(key, QUERIES, 7).astype(jnp.bfloat16)


def draw_passages(key, part):
    return cluster_rows(key, PASSAGES, 9).astype(jnp.bfloat16)


def counts_helper(key):
    return jax.random.randint(jax.random.fold_in(key, 11), (NBLOCKS,), BR // 8, BR + 1).astype(jnp.int32)


def draw_block_valid_counts(key, part):
    return counts_helper(key)


def draw_positive_index(key, part):
    counts = counts_helper(key)
    key_block, key_row = jax.random.split(jax.random.fold_in(key, 13), 2)
    chosen = jax.random.randint(key_block, (QUERIES,), 0, BPD)
    device = jnp.arange(QUERIES, dtype=jnp.int32) // QG
    top_row = counts[device * BPD + chosen]
    row = jax.random.randint(key_row, (QUERIES,), 0, top_row)
    return (chosen * BR + row).astype(jnp.int32)


def draw_neg_blocks(key, part):

    def per_device(device_key, device):
        group = device // N_REP
        replica = device % N_REP
        key_order, key_slot_positions, key_local, key_shuffle = jax.random.split(device_key, 4)
        others = jnp.arange(N_GRP - 1, dtype=jnp.int32)
        others = others + (others >= group).astype(jnp.int32)
        order = jax.random.permutation(key_order, others)
        chosen_slots = jax.random.permutation(key_slot_positions, (N_GRP - 2) * CAP)[:NEG - CAP]
        owner_group = jnp.concatenate([jnp.full((CAP,), order[0], jnp.int32), order[1:][chosen_slots // CAP]])
        slot_rank = jnp.concatenate([jnp.arange(CAP, dtype=jnp.int32), (chosen_slots % CAP).astype(jnp.int32)])
        local_table = jax.vmap(lambda sub_key: jax.random.permutation(sub_key, BPD))(jax.random.split(key_local, N_GRP))
        local_block = local_table[owner_group, slot_rank]
        global_block = (owner_group * N_REP + replica) * BPD + local_block
        return jax.random.permutation(key_shuffle, global_block).astype(jnp.int32)
    device_keys = jax.random.split(jax.random.fold_in(key, 17), N_GRP * N_REP)
    return jax.vmap(per_device)(device_keys, jnp.arange(N_GRP * N_REP, dtype=jnp.int32))


def draw_query_weights(key, part):
    position = jnp.arange(QUERIES, dtype=jnp.float32)
    ramp = 1.0 + 2.0 * position / (QUERIES - 1)
    base = jnp.exp(jax.random.uniform(jax.random.fold_in(key, 19), (QUERIES,), jnp.float32, -1.2, 1.2))
    return base * ramp


def setup_inputs(seed: int = 0) -> dict:
    streams_of = jax.random.split(jax.random.key(seed), 7)
    return {
        "queries": draw_queries(jax.random.fold_in(streams_of[6], 71), 0),
        "passages": draw_passages(jax.random.fold_in(streams_of[6], 71), 0),
        "block_valid_counts": draw_block_valid_counts(jax.random.fold_in(streams_of[6], 71), 0),
        "positive_index": draw_positive_index(jax.random.fold_in(streams_of[6], 71), 0),
        "neg_blocks": draw_neg_blocks(jax.random.fold_in(streams_of[6], 71), 0),
        "query_weights": draw_query_weights(jax.random.fold_in(streams_of[6], 71), 0),
    }


inverse_softmax_sharpness = 20.0
norm_epsilon = 1e-06

def normalize(rows):
    values = rows.astype(jnp.float32)
    scale = lax.rsqrt(lax.optimization_barrier(jnp.sum(values * values, axis=-1, keepdims=True)) + norm_epsilon)
    return (values * scale).astype(jnp.bfloat16)

def reference(queries, passages, block_valid_counts, positive_index, neg_blocks, query_weights):
    local_rows = BPD * BR
    all_blocks = passages.reshape(NBLOCKS, BR, D)

    def per_device(device):
        question_unit_vectors = normalize(lax.dynamic_slice_in_dim(queries, device * QG, QG, 0))
        document_unit_vectors = normalize(lax.dynamic_slice_in_dim(passages, device * local_rows, local_rows, 0))
        own_counts = lax.dynamic_slice_in_dim(block_valid_counts, device * BPD, BPD, 0)
        row_valid = jnp.arange(local_rows, dtype=jnp.int32) % BR < jnp.repeat(own_counts, BR)
        shared_pool_similarity = jnp.dot(question_unit_vectors, document_unit_vectors.T, preferred_element_type=jnp.float32) * inverse_softmax_sharpness
        local_total = lax.optimization_barrier(jnp.sum(jnp.where(row_valid[None, :], jnp.exp(shared_pool_similarity), 0.0), axis=1))
        positives = lax.dynamic_slice_in_dim(positive_index, device * QG, QG, 0)
        positive_score = jnp.take_along_axis(shared_pool_similarity, positives[:, None], axis=1)[:, 0]
        wanted = neg_blocks[device]
        distractor_unit_vectors = normalize(all_blocks[wanted]).reshape(NEG * BR, D)
        hard_valid = jnp.arange(NEG * BR, dtype=jnp.int32) % BR < jnp.repeat(block_valid_counts[wanted], BR)
        distractor_similarity = jnp.dot(question_unit_vectors, distractor_unit_vectors.T, preferred_element_type=jnp.float32) * inverse_softmax_sharpness
        hard_total = lax.optimization_barrier(jnp.sum(jnp.where(hard_valid[None, :], jnp.exp(distractor_similarity), 0.0), axis=1))
        return jnp.log(local_total + hard_total) - positive_score
    query_loss = lax.map(per_device, jnp.arange(N_GRP * N_REP, dtype=jnp.int32)).reshape(QUERIES)
    mean_loss = jnp.sum(query_weights * query_loss) / jnp.sum(query_weights)
    return (query_loss, mean_loss)
```

```python
import jax
import jax.numpy as jnp
from jax import lax
from jax.experimental import pallas as pl
from jax.experimental.pallas import tpu as pltpu
from jax.sharding import Mesh
from jax.sharding import PartitionSpec as P


SIDE = "grp_0"
RING = "grp_1"
CORE = "grp_2"
PLANE = ("grp_0", "grp_1")
GRP_REP = ("grp_0", "grp_1", "grp_2", "rep_0", "rep_1")

inverse_softmax_sharpness = 20.0
norm_epsilon = 1e-06
LOCAL_BLOCKS = 2
SLOTS = 2

NT = (((1,), (1,)), ((), ()))
NEIGHBOURS = ((0, -1), (0, 1), (1, 0), (1, -1), (1, 1), (0, 2), (1, 2))


def normalize(rows):
    values = rows.astype(jnp.float32)
    scale = lax.rsqrt(jnp.sum(values * values, axis=-1, keepdims=True) + norm_epsilon)
    return (values * scale).astype(jnp.bfloat16)


def units_kernel(queries, first, second, pair, third):
    rows = first.shape[0]
    for k, piece in enumerate((first, second, third)):
        unit = normalize(queries[k * rows : (k + 1) * rows, :])
        piece[...] = unit
        if k < 2:
            pair[k * rows : (k + 1) * rows, :] = unit


def query_units(queries):
    rows, width = queries.shape
    third = rows // 3
    shape = lambda n: jax.ShapeDtypeStruct((n, width), jnp.bfloat16)
    return pl.pallas_call(
        units_kernel,
        out_shape=[shape(third), shape(third), shape(2 * third), shape(third)],
        cost_estimate=pl.CostEstimate(
            flops=3 * rows * width, transcendentals=rows, bytes_accessed=6 * rows * width
        ),
        name="query_units",
    )(queries)


def local_kernel(counts, pair, third, positive, passages, units, total, score, questions):
    step = pl.program_id(0)
    rows = passages.shape[0]
    block_rows = rows // LOCAL_BLOCKS

    @pl.when(step == 0)
    def _():
        questions[: pair.shape[0], :] = pair[...]
        questions[pair.shape[0] :, :] = third[...]
        total[...] = jnp.zeros_like(total)
        score[...] = jnp.zeros_like(score)

    units[...] = normalize(passages[...])
    similarity = (
        lax.dot_general(units[...], questions[...], NT, preferred_element_type=jnp.float32)
        * inverse_softmax_sharpness
    )
    row = lax.broadcasted_iota(jnp.int32, similarity.shape, 0)
    score[...] += jnp.sum(
        jnp.where(row + step * rows == positive[...], similarity, 0.0), axis=0, keepdims=True
    )
    kept = jnp.exp(similarity)
    for k in range(LOCAL_BLOCKS):
        part = slice(k * block_rows, (k + 1) * block_rows)
        inside = row[:block_rows] < counts[step * LOCAL_BLOCKS + k]
        total[...] += jnp.sum(jnp.where(inside, kept[part], 0.0), axis=0, keepdims=True)


def score_local(counts, pair, third, positive, passages):
    local_rows, width = passages.shape
    blocks = counts.shape[0]
    step_rows = local_rows // blocks * LOCAL_BLOCKS
    steps = blocks // LOCAL_BLOCKS
    rows = positive.shape[1]
    piece = lambda a: pl.BlockSpec(a.shape, lambda s, c: (0, 0))
    line = pl.BlockSpec((1, rows), lambda s, c: (0, 0))
    band = pl.BlockSpec((step_rows, width), lambda s, c: (s, 0))
    return pl.pallas_call(
        local_kernel,
        grid_spec=pltpu.PrefetchScalarGridSpec(
            num_scalar_prefetch=1,
            grid=(steps,),
            in_specs=[piece(pair), piece(third), line, band],
            out_specs=[band, line, line],
            scratch_shapes=[pltpu.VMEM((rows, width), jnp.bfloat16)],
        ),
        out_shape=[
            jax.ShapeDtypeStruct(passages.shape, jnp.bfloat16),
            jax.ShapeDtypeStruct((1, rows), jnp.float32),
            jax.ShapeDtypeStruct((1, rows), jnp.float32),
        ],
        cost_estimate=pl.CostEstimate(
            flops=2 * local_rows * width * rows,
            transcendentals=local_rows * rows,
            bytes_accessed=4 * local_rows * width,
        ),
        name="score_local",
    )(counts, pair, third, positive, passages)


def listed_kernel(jobs, early, table, *refs):
    pieces = refs[: sum(len(job) for job in jobs)]
    done = refs[len(pieces) : len(pieces) + len(early)]
    mine, twin = refs[len(pieces) + len(early) :][:2]
    totals = refs[len(pieces) + len(early) + 2 : -2]
    keys, sems = refs[-2:]
    block_rows = mine.shape[1]

    def copies(j, source):
        found = []
        for s in range(2 * SLOTS):
            home = mine if s < SLOTS else twin
            found.append(
                pltpu.make_async_copy(
                    home.at[table[source * 4 * SLOTS + s]],
                    keys.at[j, pl.ds(s * block_rows, block_rows)],
                    sems.at[j, s],
                )
            )
        return found

    sources = [job[0][0] for job in jobs]
    started = [copies(j, source) for j, source in enumerate(sources)]
    for group in started:
        for copy in group:
            copy.start()
    for k, (j, first) in enumerate(early):
        totals[j][:, first : first + done[k].shape[1]] = done[k][...]
    at = 0
    for j, job in enumerate(jobs):
        for copy in started[j]:
            copy.wait()
        for source, first in job:
            piece = pieces[at]
            at += 1
            similarity = (
                lax.dot_general(keys[j], piece[...], NT, preferred_element_type=jnp.float32)
                * inverse_softmax_sharpness
            )
            kept = jnp.exp(similarity)
            row = lax.broadcasted_iota(jnp.int32, (block_rows, piece.shape[0]), 0)
            added = jnp.zeros((1, piece.shape[0]), jnp.float32)
            for s in range(2 * SLOTS):
                inside = row < table[source * 4 * SLOTS + 2 * SLOTS + s]
                part = kept[s * block_rows : (s + 1) * block_rows]
                added += jnp.sum(jnp.where(inside, part, 0.0), axis=0, keepdims=True)
            totals[j][:, first : first + piece.shape[0]] = added


def score_listed(table, mine, twin, jobs, early=()):
    plan, pieces, sizes = [], [], []
    taken = {}
    for k, first, line in early:
        taken[k] = max(taken.get(k, 0), first + line.shape[1])
    for j, (source, job) in enumerate(jobs):
        first = taken.get(j, 0)
        rows = []
        for piece in job:
            rows.append((source, first))
            pieces.append(piece)
            first += piece.shape[0]
        plan.append(tuple(rows))
        sizes.append(first)
    width = mine.shape[2]
    block_rows = mine.shape[1]
    amount = sum(piece.shape[0] for piece in pieces)
    vmem = pl.BlockSpec(memory_space=pltpu.VMEM)
    hbm = pl.BlockSpec(memory_space=pltpu.HBM)
    kernel = lambda *refs: listed_kernel(plan, [(j, first) for j, first, _ in early], *refs)
    return pl.pallas_call(
        kernel,
        in_specs=[pl.BlockSpec(memory_space=pltpu.SMEM)]
        + [vmem] * (len(pieces) + len(early))
        + [hbm, hbm],
        out_specs=[vmem] * len(jobs),
        out_shape=[jax.ShapeDtypeStruct((1, n), jnp.float32) for n in sizes],
        scratch_shapes=[
            pltpu.VMEM((len(jobs), 2 * SLOTS * block_rows, width), jnp.bfloat16),
            pltpu.SemaphoreType.DMA((len(jobs), 2 * SLOTS)),
        ],
        cost_estimate=pl.CostEstimate(
            flops=4 * SLOTS * block_rows * width * amount,
            transcendentals=2 * SLOTS * block_rows * amount,
            bytes_accessed=len(jobs) * 4 * SLOTS * block_rows * width + 2 * amount * width,
        ),
        name="score_listed",
    )(table, *pieces, *[line for _, _, line in early], mine, twin)


def slot_table(lists, device, blocks_here, counts):
    owner = lists // blocks_here
    block = lists % blocks_here
    mine = owner == device
    first = jnp.max(jnp.where(mine, block, -1), axis=1)
    second = jnp.min(jnp.where(mine, block, blocks_here), axis=1)
    second = jnp.where(jnp.sum(mine, axis=1) > 1, second, -1)
    index = jnp.stack([first, second], axis=1)
    choice = index[:, :, None] == jnp.arange(blocks_here, dtype=jnp.int32)[None, None, :]
    kept = jnp.sum(jnp.where(choice, counts[None, None, :], 0), axis=2)
    return jnp.maximum(index, 0), kept


def local(queries, passages, block_valid_counts, positive_index, neg_blocks, query_weights):
    _, width = queries.shape
    blocks_here = block_valid_counts.shape[0]
    ring = lax.axis_size(RING)
    replicas = lax.axis_size("rep_0") * lax.axis_size("rep_1")
    device = lax.axis_index(GRP_REP)

    def forward(a):
        return lax.ppermute(a, RING, [(i, (i + 1) % ring) for i in range(ring)])

    def backward(a):
        return lax.ppermute(a, RING, [(i, (i - 1) % ring) for i in range(ring)])

    def across(a):
        return lax.ppermute(a, SIDE, [(0, 1), (1, 0)])

    def swap(a):
        return lax.ppermute(a, CORE, [(0, 1), (1, 0)])

    def home(a, dx, dz):
        pairs = []
        for i in range(2 * ring):
            x, z = divmod(i, ring)
            pairs.append((i, (x ^ dx) * ring + (z + dz) % ring))
        return lax.ppermute(a, PLANE, pairs)

    a, b, ab, c = query_units(queries)
    below_a = forward(a)
    above_ab = backward(ab)
    beside_c = across(c)
    lists = [neg_blocks]
    for dx, dz in NEIGHBOURS:
        lists.append(home(neg_blocks, dx, -dz))
    twin_counts = swap(block_valid_counts)
    below_b = forward(b)
    below_c = forward(c)
    above_c = backward(c)
    beside_ab = across(ab)

    beside_below_a = across(below_a)
    beside_below_b = across(below_b)
    beside_above_ab = across(above_ab)
    beside_below_c = forward(beside_c)
    beside_above_c = backward(beside_c)
    facing_c = forward(below_c)
    facing_ab = backward(above_ab)
    beside_facing_a = forward(beside_below_a)
    beside_facing_b = forward(beside_below_b)
    beside_facing_c = backward(beside_above_c)

    positive = positive_index[None, :]
    units, local_total, positive_score = score_local(block_valid_counts, ab, c, positive, passages)
    blocks = units.reshape(blocks_here, -1, width)
    twin = swap(blocks)

    listed = jnp.concatenate(lists, axis=0)
    index_mine, kept_mine = slot_table(listed, device, blocks_here, block_valid_counts)
    index_twin, kept_twin = slot_table(listed, device ^ replicas, blocks_here, twin_counts)
    table = jnp.concatenate([index_mine, index_twin, kept_mine, kept_twin], axis=1).reshape(-1)

    def score(jobs, early=()):
        return score_listed(table, blocks, twin, jobs, early)

    (own_total,) = score([(0, [ab, c])])
    (total_1,) = score([(1, [below_a, below_b, below_c])])
    (total_2,) = score([(2, [above_ab, above_c])])
    (total_3,) = score([(3, [beside_ab, beside_c])])
    (total_4,) = score([(4, [beside_below_a, beside_below_b, beside_below_c])])
    (total_6,) = score([(6, [facing_ab, facing_c])])
    (early_7,) = score([(7, [beside_facing_a])])
    total_5, total_7 = score(
        [(5, [beside_above_ab, beside_above_c]), (7, [beside_facing_b, beside_facing_c])],
        [(1, 0, early_7)],
    )
    totals = [total_1, total_2, total_3, total_4, total_5, total_6, total_7]
    total = local_total + own_total
    for k, (dx, dz) in enumerate(NEIGHBOURS):
        total += home(totals[k], dx, dz)
    query_loss = (jnp.log(total) - positive_score)[0]
    sums = jnp.stack([jnp.sum(query_weights * query_loss), jnp.sum(query_weights)])
    everyone = lax.axis_size(GRP_REP)
    shares = lax.all_to_all(
        jnp.broadcast_to(sums[None, :], (everyone, 2)),
        GRP_REP,
        split_axis=0,
        concat_axis=0,
        tiled=True,
    )
    sums = jnp.sum(shares, axis=0)
    return (query_loss, sums[0] / sums[1])


def solution(mesh):
    split = Mesh(mesh.devices.reshape(2, 4, 2, 4, 2), GRP_REP)
    in_specs = (
        P(GRP_REP, None),
        P(GRP_REP, None),
        P(GRP_REP),
        P(GRP_REP),
        P(GRP_REP, None),
        P(GRP_REP),
    )
    out_specs = (P(GRP_REP), P())

    return jax.shard_map(local, mesh=split, in_specs=in_specs, out_specs=out_specs, check_vma=False)
```

```python
import jax
import jax.numpy as jnp
from jax import lax
from jax.experimental import pallas as pl
from jax.experimental.pallas import tpu as pltpu
from jax.sharding import Mesh
from jax.sharding import PartitionSpec as P


RING = "grp_1"
CORE = "grp_2"
PLANE = ("grp_0", "grp_1")
GRP_REP = ("grp_0", "grp_1", "grp_2", "rep_0", "rep_1")

inverse_softmax_sharpness = 20.0
norm_epsilon = 1e-06
LOCAL_BLOCKS = 2
PIECES = 3
EXTRA = 16
LOCAL_LIMIT = 56
SLOTS = 2

NT = (((1,), (1,)), ((), ()))


def normalize(rows):
    values = rows.astype(jnp.float32)
    scale = lax.rsqrt(jnp.sum(values * values, axis=-1, keepdims=True) + norm_epsilon)
    return (values * scale).astype(jnp.bfloat16)


def units_kernel(queries, *pieces):
    at = 0
    for piece in pieces:
        rows = piece.shape[0]
        piece[...] = normalize(queries[at : at + rows, :])
        at += rows


def query_units(queries, start, sizes):
    width = queries.shape[1]
    rows = sum(sizes)
    return pl.pallas_call(
        units_kernel,
        grid=(1,),
        in_specs=[pl.BlockSpec((rows, width), lambda i: (start // rows, 0))],
        out_specs=[pl.BlockSpec((n, width), lambda i: (0, 0)) for n in sizes],
        out_shape=[jax.ShapeDtypeStruct((n, width), jnp.bfloat16) for n in sizes],
        cost_estimate=pl.CostEstimate(
            flops=3 * rows * width, transcendentals=rows, bytes_accessed=4 * rows * width
        ),
        compiler_params=pltpu.CompilerParams(vmem_limit_bytes=12 * 2**20),
    )(queries)


def local_kernel(counts, a, b, c, positive, passages, units, total, score, questions):
    step = pl.program_id(0)
    rows = passages.shape[0]
    block_rows = rows // LOCAL_BLOCKS

    @pl.when(step == 0)
    def _():
        at = 0
        for piece in (a, b, c):
            questions[at : at + piece.shape[0], :] = piece[...]
            at += piece.shape[0]
        total[...] = jnp.zeros_like(total)
        score[...] = jnp.zeros_like(score)

    units[...] = normalize(passages[...])
    similarity = (
        lax.dot_general(units[...], questions[...], NT, preferred_element_type=jnp.float32)
        * inverse_softmax_sharpness
    )
    row = lax.broadcasted_iota(jnp.int32, similarity.shape, 0)
    score[...] += jnp.sum(
        jnp.where(row + step * rows == positive[...], similarity, 0.0), axis=0, keepdims=True
    )
    kept = jnp.exp(similarity)
    for k in range(LOCAL_BLOCKS):
        part = slice(k * block_rows, (k + 1) * block_rows)
        inside = row[:block_rows] < counts[step * LOCAL_BLOCKS + k]
        total[...] += jnp.sum(jnp.where(inside, kept[part], 0.0), axis=0, keepdims=True)


def score_local(counts, pieces, positive, passages):
    local_rows, width = passages.shape
    blocks = counts.shape[0]
    step_rows = local_rows // blocks * LOCAL_BLOCKS
    steps = blocks // LOCAL_BLOCKS
    rows = positive.shape[1]
    piece = lambda a: pl.BlockSpec(a.shape, lambda s, c: (0, 0))
    line = pl.BlockSpec((1, rows), lambda s, c: (0, 0))
    band = pl.BlockSpec((step_rows, width), lambda s, c: (s, 0))
    return pl.pallas_call(
        local_kernel,
        grid_spec=pltpu.PrefetchScalarGridSpec(
            num_scalar_prefetch=1,
            grid=(steps,),
            in_specs=[piece(a) for a in pieces] + [line, band],
            out_specs=[band, line, line],
            scratch_shapes=[pltpu.VMEM((rows, width), jnp.bfloat16)],
        ),
        out_shape=[
            jax.ShapeDtypeStruct(passages.shape, jnp.bfloat16),
            jax.ShapeDtypeStruct((1, rows), jnp.float32),
            jax.ShapeDtypeStruct((1, rows), jnp.float32),
        ],
        cost_estimate=pl.CostEstimate(
            flops=2 * local_rows * width * rows,
            transcendentals=local_rows * rows,
            bytes_accessed=4 * local_rows * width,
        ),
        compiler_params=pltpu.CompilerParams(vmem_limit_bytes=LOCAL_LIMIT * 2**20),
        name="local",
    )(counts, *pieces, positive, passages)


def listed_kernel(jobs, table, *refs):
    refs = list(refs)
    take = lambda n: [refs.pop(0) for _ in range(n)]
    pieces = [take(count) for _, _, count, _, _ in jobs]
    given = [take(1)[0] if is_given else None for _, _, _, is_given, _ in jobs]
    mine, twin = (None, None) if all(job[3] for job in jobs) else take(2)
    totals = [take(1)[0] if count else None for _, _, count, _, _ in jobs]
    held = [take(1)[0] if keep else None for _, _, _, _, keep in jobs]
    held = [ref if job[4] or job[3] else take(1)[0] for ref, job in zip(held, jobs)]
    stacks = [take(1)[0] if count else None for _, _, count, _, _ in jobs]
    (sems,) = refs

    started = []
    for j, (source, slots, _, is_given, _) in enumerate(jobs):
        group = []
        at = 0
        for k, piece in enumerate(pieces[j]):
            target = stacks[j].at[pl.ds(at, piece.shape[0])]
            group.append(pltpu.make_async_copy(piece, target, sems.at[j, 2 * SLOTS + k]))
            at += piece.shape[0]
        for k, s in enumerate(() if is_given else slots):
            home = mine if s < SLOTS else twin
            block = home.at[table[source * 4 * SLOTS + s]]
            target = held[j].at[pl.ds(k * mine.shape[1], mine.shape[1])]
            group.append(pltpu.make_async_copy(block, target, sems.at[j, k]))
        for copy in group:
            copy.start()
        started.append(group)
    for j, (source, slots, count, is_given, _) in enumerate(jobs):
        for copy in started[j]:
            copy.wait()
        if not count:
            continue
        keys = given[j] if is_given else held[j]
        block_rows = keys.shape[0] // len(slots)
        similarity = (
            lax.dot_general(keys[...], stacks[j][...], NT, preferred_element_type=jnp.float32)
            * inverse_softmax_sharpness
        )
        kept = jnp.exp(similarity)
        row = lax.broadcasted_iota(jnp.int32, (block_rows, kept.shape[1]), 0)
        total = jnp.zeros((1, kept.shape[1]), jnp.float32)
        for k, s in enumerate(slots):
            inside = row < table[source * 4 * SLOTS + 2 * SLOTS + s]
            part = kept[k * block_rows : (k + 1) * block_rows]
            total += jnp.sum(jnp.where(inside, part, 0.0), axis=0, keepdims=True)
        totals[j][...] = total


def score_listed(table, mine, twin, rows, jobs, limit):
    width = mine.shape[2]
    block_rows = mine.shape[1]
    plan, operands = [], []
    for source, pieces, given, keep in jobs:
        slots = tuple(range(SLOTS if source == 0 else 0, 2 * SLOTS))
        plan.append((source, slots, len(pieces), given is not None, keep))
        operands += pieces
    scored = sum(job[2] > 0 for job in plan)
    given = [keys for _, _, keys, _ in jobs if keys is not None]
    held = lambda job: (len(job[1]) * block_rows, width)
    outs = [jax.ShapeDtypeStruct((1, rows), jnp.float32)] * scored
    outs += [jax.ShapeDtypeStruct(held(job), jnp.bfloat16) for job in plan if job[4]]
    scratch = [pltpu.VMEM(held(job), jnp.bfloat16) for job in plan if not (job[3] or job[4])]
    scratch += [pltpu.VMEM((rows, width), jnp.bfloat16)] * scored
    sources = [] if all(job[3] for job in plan) else [mine, twin]
    vmem = pl.BlockSpec(memory_space=pltpu.VMEM)
    hbm = pl.BlockSpec(memory_space=pltpu.HBM)
    kernel = lambda *refs: listed_kernel(plan, *refs)
    return pl.pallas_call(
        kernel,
        in_specs=[pl.BlockSpec(memory_space=pltpu.SMEM)]
        + [hbm] * len(operands)
        + [vmem] * len(given)
        + [hbm] * len(sources),
        out_specs=[vmem] * len(outs),
        out_shape=outs,
        scratch_shapes=scratch + [pltpu.SemaphoreType.DMA((len(plan), 2 * SLOTS + PIECES))],
        cost_estimate=pl.CostEstimate(
            flops=4 * SLOTS * block_rows * width * rows * scored,
            transcendentals=2 * SLOTS * block_rows * rows * scored,
            bytes_accessed=(2 * SLOTS * block_rows * len(jobs) + rows * scored) * width * 2,
        ),
        compiler_params=pltpu.CompilerParams(vmem_limit_bytes=limit * 2**20),
        name="listed",
    )(table, *operands, *given, *sources)


def last_kernel(source, count, table, *refs):
    pieces, (keys, base, *parts) = refs[:count], refs[count:-4]
    loss, shares, stack, _ = refs[-4:]
    at = 0
    for piece in pieces:
        stack[at : at + piece.shape[0], :] = piece[...]
        at += piece.shape[0]
    total = base[0:1, :]
    for part in parts:
        total += part[...]
    similarity = (
        lax.dot_general(keys[...], stack[...], NT, preferred_element_type=jnp.float32)
        * inverse_softmax_sharpness
    )
    kept = jnp.exp(similarity)
    block_rows = keys.shape[0] // (2 * SLOTS)
    row = lax.broadcasted_iota(jnp.int32, (block_rows, kept.shape[1]), 0)
    for s in range(2 * SLOTS):
        inside = row < table[source * 4 * SLOTS + 2 * SLOTS + s]
        part = kept[s * block_rows : (s + 1) * block_rows]
        total += jnp.sum(jnp.where(inside, part, 0.0), axis=0, keepdims=True)
    value = jnp.log(total) - base[1:2, :]
    loss[...] = value
    weights = base[2:3, :]
    lane = lax.broadcasted_iota(jnp.int32, shares.shape, 1)
    weighted = jnp.sum(weights * value, axis=1, keepdims=True)
    weight = jnp.sum(weights, axis=1, keepdims=True)
    shares[...] = jnp.where(lane == 0, weighted, weight)


def score_last(table, source, pieces, keys, base, parts, everyone):
    rows = base.shape[1]
    width = keys.shape[1]
    vmem = pl.BlockSpec(memory_space=pltpu.VMEM)
    hbm = pl.BlockSpec(memory_space=pltpu.HBM)
    kernel = lambda *refs: last_kernel(source, len(pieces), *refs)
    return pl.pallas_call(
        kernel,
        in_specs=[pl.BlockSpec(memory_space=pltpu.SMEM)]
        + [vmem] * len(pieces)
        + [vmem] * (2 + len(parts)),
        out_specs=[vmem, vmem],
        out_shape=[
            jax.ShapeDtypeStruct((1, rows), jnp.float32),
            jax.ShapeDtypeStruct((everyone, 2), jnp.float32),
        ],
        scratch_shapes=[
            pltpu.VMEM((rows, width), jnp.bfloat16),
            pltpu.SemaphoreType.DMA((len(pieces),)),
        ],
        cost_estimate=pl.CostEstimate(
            flops=2 * keys.shape[0] * width * rows,
            transcendentals=keys.shape[0] * rows,
            bytes_accessed=2 * (keys.shape[0] + rows) * width,
        ),
        compiler_params=pltpu.CompilerParams(vmem_limit_bytes=12 * 2**20),
        name="last",
    )(table, *pieces, keys, base, *parts)


def slot_table(lists, device, blocks_here, counts):
    owner = lists // blocks_here
    block = lists % blocks_here
    mine = owner == device
    first = jnp.max(jnp.where(mine, block, -1), axis=1)
    second = jnp.min(jnp.where(mine, block, blocks_here), axis=1)
    second = jnp.where(jnp.sum(mine, axis=1) > 1, second, -1)
    index = jnp.stack([first, second], axis=1)
    choice = index[:, :, None] == jnp.arange(blocks_here, dtype=jnp.int32)[None, None, :]
    kept = jnp.sum(jnp.where(choice, counts[None, None, :], 0), axis=2)
    return jnp.maximum(index, 0), kept


def local(queries, passages, block_valid_counts, positive_index, neg_blocks, query_weights):
    rows, width = queries.shape
    blocks_here = block_valid_counts.shape[0]
    ring = lax.axis_size(RING)
    replicas = lax.axis_size("rep_0") * lax.axis_size("rep_1")
    device = lax.axis_index(GRP_REP)

    def shift(a, dx, dz):
        pairs = []
        for i in range(2 * ring):
            x, z = divmod(i, ring)
            pairs.append((i, (x ^ dx) * ring + (z + dz) % ring))
        return lax.ppermute(a, PLANE, pairs)

    forward = lambda a: shift(a, 0, 1)
    backward = lambda a: shift(a, 0, -1)
    across = lambda a: shift(a, 1, 0)

    def swap(a):
        return lax.ppermute(a, CORE, [(0, 1), (1, 0)])

    pair = jnp.concatenate([neg_blocks, across(neg_blocks)], axis=0)
    rows_c = rows // PIECES
    rows_a = rows_c + EXTRA
    (c,) = query_units(queries[rows - rows_c :], 0, [rows_c])
    a, b = query_units(queries, 0, [rows_a, rows - rows_c - rows_a])
    beside_c = across(c)
    below_c = forward(c)
    above_c = backward(c)
    pair_below = forward(pair)
    pair_above = backward(pair)
    beside_b = across(b)
    below_a = forward(a)
    above_a = backward(a)
    beside_a = across(a)
    below_b = forward(b)
    above_b = backward(b)
    twin_counts = swap(block_valid_counts)
    pair_facing = forward(pair_below)

    beside_below_c = forward(beside_c)
    facing_c = backward(above_c)
    beside_below_a = across(below_a)
    facing_a = forward(below_a)
    beside_above_b = backward(beside_b)
    beside_below_b = across(below_b)
    beside_above_c = across(above_c)
    facing_b = forward(below_b)
    beside_above_a = backward(beside_a)
    beside_facing_c = forward(beside_below_c)
    beside_facing_a = across(facing_a)
    beside_facing_b = backward(beside_above_b)

    positive = positive_index[None, :]
    units, local_total, positive_score = score_local(
        block_valid_counts, (a, b, c), positive, passages
    )
    blocks = units.reshape(blocks_here, -1, width)
    twin = swap(blocks)

    def slots(lists):
        listed = jnp.concatenate(lists, axis=0)
        index_mine, kept_mine = slot_table(listed, device, blocks_here, block_valid_counts)
        index_twin, kept_twin = slot_table(listed, device ^ replicas, blocks_here, twin_counts)
        return jnp.concatenate([index_mine, index_twin, kept_mine, kept_twin], axis=1).reshape(-1)

    near_table = slots([pair, pair_below, pair_above])
    table = jnp.concatenate([near_table, slots([pair_facing])])

    def score(table, jobs, limit):
        return score_listed(table, blocks, twin, rows, jobs, limit)

    own_total, beside_total, below_total, above_total = score(
        near_table,
        [
            (0, [a, b, c], None, False),
            (1, [beside_a, beside_b, beside_c], None, False),
            (2, [below_a, below_b, below_c], None, False),
            (4, [above_a, above_b, above_c], None, False),
        ],
        56,
    )
    beside_below_total, keys = score(
        table,
        [
            (3, [beside_below_a, beside_below_b, beside_below_c], None, False),
            (7, [], None, True),
        ],
        56,
    )
    facing_total, beside_above_total = score(
        table,
        [
            (6, [facing_a, facing_b, facing_c], None, False),
            (5, [beside_above_a, beside_above_b, beside_above_c], None, False),
        ],
        56,
    )
    half = ring // 2
    base = jnp.concatenate([local_total + own_total, positive_score, query_weights[None, :]])
    base = shift(base, 1, half)
    parts = [
        shift(beside_total, 0, half),
        shift(below_total, 1, half - 1),
        shift(above_total, 1, half + 1),
        shift(beside_below_total, 0, half - 1),
        shift(facing_total, 1, 0),
        shift(beside_above_total, 0, half + 1),
    ]
    query_loss, shares = score_last(
        table,
        7,
        [beside_facing_a, beside_facing_b, beside_facing_c],
        keys,
        base,
        parts,
        lax.axis_size(GRP_REP),
    )
    query_loss = shift(query_loss[0], 1, half)
    shares = lax.all_to_all(shares, GRP_REP, split_axis=0, concat_axis=0, tiled=True)
    sums = jnp.sum(shares, axis=0)
    return (query_loss, sums[0] / sums[1])


def solution(mesh):
    split = Mesh(mesh.devices.reshape(2, 4, 2, 4, 2), GRP_REP)
    in_specs = (
        P(GRP_REP, None),
        P(GRP_REP, None),
        P(GRP_REP),
        P(GRP_REP),
        P(GRP_REP, None),
        P(GRP_REP),
    )
    out_specs = (P(GRP_REP), P())

    return jax.shard_map(local, mesh=split, in_specs=in_specs, out_specs=out_specs, check_vma=False)
```

```python
import jax
import jax.numpy as jnp
from jax import lax
from jax.experimental import pallas as pl
from jax.experimental.pallas import tpu as pltpu
from jax.sharding import Mesh
from jax.sharding import PartitionSpec as P


RING = "grp_1"
CORE = "grp_2"
PLANE = ("grp_0", "grp_1")
GRP_REP = ("grp_0", "grp_1", "grp_2", "rep_0", "rep_1")

inverse_softmax_sharpness = 20.0
norm_epsilon = 1e-06
LOCAL_BLOCKS = 2
PIECES = 3
EXTRA = 16
LOCAL_LIMIT = 56
SLOTS = 2

NT = (((1,), (1,)), ((), ()))


def normalize(rows):
    values = rows.astype(jnp.float32)
    scale = lax.rsqrt(jnp.sum(values * values, axis=-1, keepdims=True) + norm_epsilon)
    return (values * scale).astype(jnp.bfloat16)


def units_kernel(queries, *pieces):
    at = 0
    for piece in pieces:
        rows = piece.shape[0]
        piece[...] = normalize(queries[at : at + rows, :])
        at += rows


def query_units(queries, start, sizes):
    width = queries.shape[1]
    rows = sum(sizes)
    return pl.pallas_call(
        units_kernel,
        grid=(1,),
        in_specs=[pl.BlockSpec((rows, width), lambda i: (start // rows, 0))],
        out_specs=[pl.BlockSpec((n, width), lambda i: (0, 0)) for n in sizes],
        out_shape=[jax.ShapeDtypeStruct((n, width), jnp.bfloat16) for n in sizes],
        cost_estimate=pl.CostEstimate(
            flops=3 * rows * width, transcendentals=rows, bytes_accessed=4 * rows * width
        ),
        compiler_params=pltpu.CompilerParams(vmem_limit_bytes=12 * 2**20),
    )(queries)


def local_kernel(counts, a, b, c, positive, passages, units, total, score, questions):
    step = pl.program_id(0)
    rows = passages.shape[0]
    block_rows = rows // LOCAL_BLOCKS

    @pl.when(step == 0)
    def _():
        at = 0
        for piece in (a, b, c):
            questions[at : at + piece.shape[0], :] = piece[...]
            at += piece.shape[0]
        total[...] = jnp.zeros_like(total)
        score[...] = jnp.zeros_like(score)

    units[...] = normalize(passages[...])
    similarity = (
        lax.dot_general(units[...], questions[...], NT, preferred_element_type=jnp.float32)
        * inverse_softmax_sharpness
    )
    row = lax.broadcasted_iota(jnp.int32, similarity.shape, 0)
    score[...] += jnp.sum(
        jnp.where(row + step * rows == positive[...], similarity, 0.0), axis=0, keepdims=True
    )
    kept = jnp.exp(similarity)
    for k in range(LOCAL_BLOCKS):
        part = slice(k * block_rows, (k + 1) * block_rows)
        inside = row[:block_rows] < counts[step * LOCAL_BLOCKS + k]
        total[...] += jnp.sum(jnp.where(inside, kept[part], 0.0), axis=0, keepdims=True)


def score_local(counts, pieces, positive, passages):
    local_rows, width = passages.shape
    blocks = counts.shape[0]
    step_rows = local_rows // blocks * LOCAL_BLOCKS
    steps = blocks // LOCAL_BLOCKS
    rows = positive.shape[1]
    piece = lambda a: pl.BlockSpec(a.shape, lambda s, c: (0, 0))
    line = pl.BlockSpec((1, rows), lambda s, c: (0, 0))
    band = pl.BlockSpec((step_rows, width), lambda s, c: (s, 0))
    return pl.pallas_call(
        local_kernel,
        grid_spec=pltpu.PrefetchScalarGridSpec(
            num_scalar_prefetch=1,
            grid=(steps,),
            in_specs=[piece(a) for a in pieces] + [line, band],
            out_specs=[band, line, line],
            scratch_shapes=[pltpu.VMEM((rows, width), jnp.bfloat16)],
        ),
        out_shape=[
            jax.ShapeDtypeStruct(passages.shape, jnp.bfloat16),
            jax.ShapeDtypeStruct((1, rows), jnp.float32),
            jax.ShapeDtypeStruct((1, rows), jnp.float32),
        ],
        cost_estimate=pl.CostEstimate(
            flops=2 * local_rows * width * rows,
            transcendentals=local_rows * rows,
            bytes_accessed=4 * local_rows * width,
        ),
        compiler_params=pltpu.CompilerParams(vmem_limit_bytes=LOCAL_LIMIT * 2**20),
        name="local",
    )(counts, *pieces, positive, passages)


def listed_kernel(jobs, table, *refs):
    refs = list(refs)
    take = lambda n: [refs.pop(0) for _ in range(n)]
    pieces = [take(count) for _, _, count, _, _ in jobs]
    given = [take(1)[0] if is_given else None for _, _, _, is_given, _ in jobs]
    mine, twin = (None, None) if all(job[3] for job in jobs) else take(2)
    totals = [take(1)[0] if count else None for _, _, count, _, _ in jobs]
    held = [take(1)[0] if keep else None for _, _, _, _, keep in jobs]
    held = [ref if job[4] or job[3] else take(1)[0] for ref, job in zip(held, jobs)]
    stacks = [take(1)[0] if count else None for _, _, count, _, _ in jobs]
    (sems,) = refs

    started = []
    for j, (source, slots, _, is_given, _) in enumerate(jobs):
        group = []
        at = 0
        for k, piece in enumerate(pieces[j]):
            target = stacks[j].at[pl.ds(at, piece.shape[0])]
            group.append(pltpu.make_async_copy(piece, target, sems.at[j, 2 * SLOTS + k]))
            at += piece.shape[0]
        for k, s in enumerate(() if is_given else slots):
            home = mine if s < SLOTS else twin
            block = home.at[table[source * 4 * SLOTS + s]]
            target = held[j].at[pl.ds(k * mine.shape[1], mine.shape[1])]
            group.append(pltpu.make_async_copy(block, target, sems.at[j, k]))
        for copy in group:
            copy.start()
        started.append(group)
    for j, (source, slots, count, is_given, _) in enumerate(jobs):
        for copy in started[j]:
            copy.wait()
        if not count:
            continue
        keys = given[j] if is_given else held[j]
        block_rows = keys.shape[0] // len(slots)
        similarity = (
            lax.dot_general(keys[...], stacks[j][...], NT, preferred_element_type=jnp.float32)
            * inverse_softmax_sharpness
        )
        kept = jnp.exp(similarity)
        row = lax.broadcasted_iota(jnp.int32, (block_rows, kept.shape[1]), 0)
        total = jnp.zeros((1, kept.shape[1]), jnp.float32)
        for k, s in enumerate(slots):
            inside = row < table[source * 4 * SLOTS + 2 * SLOTS + s]
            part = kept[k * block_rows : (k + 1) * block_rows]
            total += jnp.sum(jnp.where(inside, part, 0.0), axis=0, keepdims=True)
        totals[j][...] = total


def score_listed(table, mine, twin, rows, jobs, limit):
    width = mine.shape[2]
    block_rows = mine.shape[1]
    plan, operands = [], []
    for source, pieces, given, keep in jobs:
        slots = tuple(range(SLOTS if source == 0 else 0, 2 * SLOTS))
        plan.append((source, slots, len(pieces), given is not None, keep))
        operands += pieces
    scored = sum(job[2] > 0 for job in plan)
    given = [keys for _, _, keys, _ in jobs if keys is not None]
    held = lambda job: (len(job[1]) * block_rows, width)
    outs = [jax.ShapeDtypeStruct((1, rows), jnp.float32)] * scored
    outs += [jax.ShapeDtypeStruct(held(job), jnp.bfloat16) for job in plan if job[4]]
    scratch = [pltpu.VMEM(held(job), jnp.bfloat16) for job in plan if not (job[3] or job[4])]
    scratch += [pltpu.VMEM((rows, width), jnp.bfloat16)] * scored
    sources = [] if all(job[3] for job in plan) else [mine, twin]
    vmem = pl.BlockSpec(memory_space=pltpu.VMEM)
    hbm = pl.BlockSpec(memory_space=pltpu.HBM)
    kernel = lambda *refs: listed_kernel(plan, *refs)
    return pl.pallas_call(
        kernel,
        in_specs=[pl.BlockSpec(memory_space=pltpu.SMEM)]
        + [hbm] * len(operands)
        + [vmem] * len(given)
        + [hbm] * len(sources),
        out_specs=[vmem] * len(outs),
        out_shape=outs,
        scratch_shapes=scratch + [pltpu.SemaphoreType.DMA((len(plan), 2 * SLOTS + PIECES))],
        cost_estimate=pl.CostEstimate(
            flops=4 * SLOTS * block_rows * width * rows * scored,
            transcendentals=2 * SLOTS * block_rows * rows * scored,
            bytes_accessed=(2 * SLOTS * block_rows * len(jobs) + rows * scored) * width * 2,
        ),
        compiler_params=pltpu.CompilerParams(vmem_limit_bytes=limit * 2**20),
        name="listed",
    )(table, *operands, *given, *sources)


def last_kernel(source, count, table, *refs):
    pieces, (keys, base, *parts) = refs[:count], refs[count:-4]
    loss, shares, stack, _ = refs[-4:]
    at = 0
    for piece in pieces:
        stack[at : at + piece.shape[0], :] = piece[...]
        at += piece.shape[0]
    total = base[0:1, :]
    for part in parts:
        total += part[...]
    similarity = (
        lax.dot_general(keys[...], stack[...], NT, preferred_element_type=jnp.float32)
        * inverse_softmax_sharpness
    )
    kept = jnp.exp(similarity)
    block_rows = keys.shape[0] // (2 * SLOTS)
    row = lax.broadcasted_iota(jnp.int32, (block_rows, kept.shape[1]), 0)
    for s in range(2 * SLOTS):
        inside = row < table[source * 4 * SLOTS + 2 * SLOTS + s]
        part = kept[s * block_rows : (s + 1) * block_rows]
        total += jnp.sum(jnp.where(inside, part, 0.0), axis=0, keepdims=True)
    value = jnp.log(total) - base[1:2, :]
    loss[...] = value
    weights = base[2:3, :]
    lane = lax.broadcasted_iota(jnp.int32, shares.shape, 1)
    weighted = jnp.sum(weights * value, axis=1, keepdims=True)
    weight = jnp.sum(weights, axis=1, keepdims=True)
    shares[...] = jnp.where(lane == 0, weighted, weight)


def score_last(table, source, pieces, keys, base, parts, everyone):
    rows = base.shape[1]
    width = keys.shape[1]
    vmem = pl.BlockSpec(memory_space=pltpu.VMEM)
    hbm = pl.BlockSpec(memory_space=pltpu.HBM)
    kernel = lambda *refs: last_kernel(source, len(pieces), *refs)
    return pl.pallas_call(
        kernel,
        in_specs=[pl.BlockSpec(memory_space=pltpu.SMEM)]
        + [vmem] * len(pieces)
        + [vmem] * (2 + len(parts)),
        out_specs=[vmem, vmem],
        out_shape=[
            jax.ShapeDtypeStruct((1, rows), jnp.float32),
            jax.ShapeDtypeStruct((everyone, 2), jnp.float32),
        ],
        scratch_shapes=[
            pltpu.VMEM((rows, width), jnp.bfloat16),
            pltpu.SemaphoreType.DMA((len(pieces),)),
        ],
        cost_estimate=pl.CostEstimate(
            flops=2 * keys.shape[0] * width * rows,
            transcendentals=keys.shape[0] * rows,
            bytes_accessed=2 * (keys.shape[0] + rows) * width,
        ),
        compiler_params=pltpu.CompilerParams(vmem_limit_bytes=12 * 2**20),
        name="last",
    )(table, *pieces, keys, base, *parts)


def mean_kernel(shares, mean):
    sums = jnp.sum(shares[...], axis=0, keepdims=True)
    mean[...] = sums[:, 0:1] / sums[:, 1:2]


def mean_of(shares):
    return pl.pallas_call(
        mean_kernel,
        out_shape=jax.ShapeDtypeStruct((1, 1), jnp.float32),
        compiler_params=pltpu.CompilerParams(vmem_limit_bytes=4 * 2**20),
        name="ratio",
    )(shares)


def slot_table(lists, device, blocks_here, counts):
    owner = lists // blocks_here
    block = lists % blocks_here
    mine = owner == device
    first = jnp.max(jnp.where(mine, block, -1), axis=1)
    second = jnp.min(jnp.where(mine, block, blocks_here), axis=1)
    second = jnp.where(jnp.sum(mine, axis=1) > 1, second, -1)
    index = jnp.stack([first, second], axis=1)
    choice = index[:, :, None] == jnp.arange(blocks_here, dtype=jnp.int32)[None, None, :]
    kept = jnp.sum(jnp.where(choice, counts[None, None, :], 0), axis=2)
    return jnp.maximum(index, 0), kept


def local(queries, passages, block_valid_counts, positive_index, neg_blocks, query_weights):
    rows, width = queries.shape
    blocks_here = block_valid_counts.shape[0]
    ring = lax.axis_size(RING)
    replicas = lax.axis_size("rep_0") * lax.axis_size("rep_1")
    device = lax.axis_index(GRP_REP)

    def shift(a, dx, dz):
        pairs = []
        for i in range(2 * ring):
            x, z = divmod(i, ring)
            pairs.append((i, (x ^ dx) * ring + (z + dz) % ring))
        return lax.ppermute(a, PLANE, pairs)

    forward = lambda a: shift(a, 0, 1)
    backward = lambda a: shift(a, 0, -1)
    across = lambda a: shift(a, 1, 0)

    def swap(a):
        return lax.ppermute(a, CORE, [(0, 1), (1, 0)])

    pair = jnp.concatenate([neg_blocks, across(neg_blocks)], axis=0)
    rows_c = rows // PIECES
    rows_a = rows_c + EXTRA
    (c,) = query_units(queries[rows - rows_c :], 0, [rows_c])
    a, b = query_units(queries, 0, [rows_a, rows - rows_c - rows_a])
    beside_c = across(c)
    below_c = forward(c)
    above_c = backward(c)
    pair_below = forward(pair)
    pair_above = backward(pair)
    beside_b = across(b)
    below_a = forward(a)
    above_a = backward(a)
    beside_a = across(a)
    below_b = forward(b)
    above_b = backward(b)
    twin_counts = swap(block_valid_counts)
    pair_facing = forward(pair_below)

    beside_below_c = forward(beside_c)
    facing_c = backward(above_c)
    beside_below_a = across(below_a)
    facing_a = forward(below_a)
    beside_above_b = backward(beside_b)
    beside_below_b = across(below_b)
    beside_above_c = across(above_c)
    facing_b = forward(below_b)
    beside_above_a = backward(beside_a)
    beside_facing_c = forward(beside_below_c)
    beside_facing_a = across(facing_a)
    beside_facing_b = backward(beside_above_b)

    positive = positive_index[None, :]
    units, local_total, positive_score = score_local(
        block_valid_counts, (a, b, c), positive, passages
    )
    blocks = units.reshape(blocks_here, -1, width)
    twin = swap(blocks)

    def slots(lists):
        listed = jnp.concatenate(lists, axis=0)
        index_mine, kept_mine = slot_table(listed, device, blocks_here, block_valid_counts)
        index_twin, kept_twin = slot_table(listed, device ^ replicas, blocks_here, twin_counts)
        return jnp.concatenate([index_mine, index_twin, kept_mine, kept_twin], axis=1).reshape(-1)

    near_table = slots([pair, pair_below, pair_above])
    table = jnp.concatenate([near_table, slots([pair_facing])])

    def score(table, jobs, limit):
        return score_listed(table, blocks, twin, rows, jobs, limit)

    own_total, beside_total, below_total, above_total = score(
        near_table,
        [
            (0, [a, b, c], None, False),
            (1, [beside_a, beside_b, beside_c], None, False),
            (2, [below_a, below_b, below_c], None, False),
            (4, [above_a, above_b, above_c], None, False),
        ],
        56,
    )
    beside_below_total, keys = score(
        table,
        [
            (3, [beside_below_a, beside_below_b, beside_below_c], None, False),
            (7, [], None, True),
        ],
        56,
    )
    facing_total, beside_above_total = score(
        table,
        [
            (6, [facing_a, facing_b, facing_c], None, False),
            (5, [beside_above_a, beside_above_b, beside_above_c], None, False),
        ],
        56,
    )
    half = ring // 2
    base = jnp.concatenate([local_total + own_total, positive_score, query_weights[None, :]])
    base = shift(base, 1, half)
    parts = [
        shift(beside_total, 0, half),
        shift(below_total, 1, half - 1),
        shift(above_total, 1, half + 1),
        shift(beside_below_total, 0, half - 1),
        shift(facing_total, 1, 0),
        shift(beside_above_total, 0, half + 1),
    ]
    query_loss, shares = score_last(
        table,
        7,
        [beside_facing_a, beside_facing_b, beside_facing_c],
        keys,
        base,
        parts,
        lax.axis_size(GRP_REP),
    )
    query_loss = shift(query_loss[0], 1, half)
    shares = lax.all_to_all(shares, GRP_REP, split_axis=0, concat_axis=0, tiled=True)
    mean = mean_of(shares)
    return (query_loss, mean[0, 0])


def solution(mesh):
    split = Mesh(mesh.devices.reshape(2, 4, 2, 4, 2), GRP_REP)
    in_specs = (
        P(GRP_REP, None),
        P(GRP_REP, None),
        P(GRP_REP),
        P(GRP_REP),
        P(GRP_REP, None),
        P(GRP_REP),
    )
    out_specs = (P(GRP_REP), P())

    return jax.shard_map(local, mesh=split, in_specs=in_specs, out_specs=out_specs, check_vma=False)
```
